32 devices in a mesh: dp: 4 (over z), hid: 2 (over x), dm: 4 (over y, core).
Axes of the slice: x: 2, y: 2, z: 4, core: 2. Of those that a mesh axis runs over, the one named last changes fastest.
Arguments:
- tokens: bfloat16 [32768, 1024], P(('dp', 'hid', 'dm')), may hold values from -6 to 6
- first_values: bfloat16 [32768, 1024], P(('dp', 'hid', 'dm')), may hold values from -6 to 6
- doc_lengths: int32 [32, 8], P(('dp', 'hid', 'dm')), may hold values from 1 to 512, 1024 in all within a row
- cotangent: bfloat16 [32768, 1024], P(('dp', 'hid', 'dm')), may hold values from -6 to 6
- attn_gain: bfloat16 [1024], P(('dp', 'hid', 'dm')), may hold values from 0.25 to 1.75
- w_query: bfloat16 [1024, 1024], P(('dp', 'hid', 'dm')), may hold values from -0.1875 to 0.1875
- w_key: bfloat16 [1024, 1024], P(('dp', 'hid', 'dm')), may hold values from -0.1875 to 0.1875
- w_value: bfloat16 [1024, 1024], P(('dp', 'hid', 'dm')), may hold values from -0.1875 to 0.1875
- w_out: bfloat16 [1024, 1024], P(('dp', 'hid', 'dm')), may hold values from -1 to 1
- mlp_gain: bfloat16 [1024], P(('dp', 'hid', 'dm')), may hold values from 0.25 to 1.75
- w_gate: bfloat16 [1024, 2816], P(None, ('hid', 'dm')), may hold values from -0.1875 to 0.1875
- w_up: bfloat16 [1024, 2816], P(None, ('hid', 'dm')), may hold values from -0.1875 to 0.1875
- w_down: bfloat16 [2816, 1024], P(('hid', 'dm')), may hold values from -0.109375 to 0.109375
Outputs:
- output: bfloat16 [32768, 1024], P(('dp', 'hid', 'dm'))
- tokens_grad: bfloat16 [32768, 1024], P(('dp', 'hid', 'dm'))
- first_values_grad: bfloat16 [32768, 1024], P(('dp', 'hid', 'dm'))
- w_query_grad: float32 [1024, 1024], P(('dp', 'hid', 'dm'))
- w_key_grad: float32 [1024, 1024], P(('dp', 'hid', 'dm'))
- w_value_grad: float32 [1024, 1024], P(('dp', 'hid', 'dm'))
- w_out_grad: float32 [1024, 1024], P(('dp', 'hid', 'dm'))
- attn_gain_grad: float32 [1024], P(('dp', 'hid', 'dm'))
- mlp_gain_grad: float32 [1024], P(('dp', 'hid', 'dm'))
- w_gate_grad: float32 [1024, 2816], P(None, ('hid', 'dm'))
- w_up_grad: float32 [1024, 2816], P(None, ('hid', 'dm'))
- w_down_grad: float32 [2816, 1024], P(('hid', 'dm'))
The draws below stay inside these ranges and needn't reach their ends.
Inputs may be any that keep to these rules, and one draw needn't show every extreme that they name: `doc_lengths`: each packed row's 8 document lengths sum to 1024, and every row holds one document of the maximum length.
All inputs are finite; a program needn't handle non-finite values.
Results may differ from the reference program's by a relative error of at most 0.017.
Values may be sent and summed in bfloat16 or wider, within the bound.
A program may use at most 192 MiB of HBM per device.

```python
import math
import jax
import jax.numpy as jnp
import numpy as np
from jax import lax

D = 1024
HEADS = 16
FF = 2816
HD = 64
ROW = 1024
NDOC = 8
ROWS = 32
TOKENS = 32768


def level_of(stream_key, extent, shards, smallest, top_value):
    def one(position, blocks):
        heights = jax.random.uniform(jax.random.fold_in(jax.random.fold_in(stream_key, 6), position), (blocks,), jnp.float32, smallest / len(shards), top_value / len(shards))
        return jnp.repeat(jnp.exp(heights), extent[position] // blocks).reshape((-1,) + (1,) * (len(extent) - position - 1))

    factor_of = one(*shards[0])
    for cut in shards[1:]:
        factor_of = factor_of * one(*cut)
    return factor_of


def profile(number_of, total, limit, slope):
    portions = [(1 << 20) // math.isqrt(grade ** slope) + 1 for grade in range(2, number_of + 1)]
    rest, counts = total - limit - (number_of - 1), [1] * (number_of - 1)
    while rest > 0:
        free = [i for i in range(number_of - 1) if counts[i] < limit]
        whole, left = sum([portions[i] for i in free]), rest
        for i in free:
            addition = min(limit - counts[i], max(1, left * portions[i] // whole), rest)
            counts[i] = counts[i] + addition
            rest = rest - addition
    return np.array([limit] + counts)


def ragged_sizes(rng, amount, total, limit, slope):
    if amount == 2:
        one = jax.random.randint(rng, (), max(1, total - limit), min(limit, total - 1) + 1)
        return jnp.stack([one, total - one])
    tallies = jnp.asarray(profile(amount, total, limit, slope), jnp.int32)
    twos = (amount - 1) // 2
    donor, receiver = tallies[1:1 + 2 * twos:2], tallies[2:2 + 2 * twos:2]
    margin = jnp.minimum(donor - 1, limit - receiver)
    shifted = jax.random.randint(jax.random.fold_in(rng, 1), (twos,), 0, 1 << 20) % (margin + 1)
    tallies = tallies.at[1:1 + 2 * twos:2].set(donor - shifted).at[2:2 + 2 * twos:2].set(receiver + shifted)
    return tallies[jax.random.permutation(jax.random.fold_in(rng, 2), amount)]


def gaussian(own_key, shape, spread, limit, shards=(), dtype=jnp.bfloat16):
    drawn = jax.random.normal(own_key, shape, jnp.float32) * spread
    if len(shards) > 0:
        drawn = level_of(own_key, shape, shards, -0.22, 0.18) * drawn
    return jnp.clip(drawn, min=-limit, max=limit).astype(dtype)


def setup_inputs(seed: int = 0) -> dict:
    key_of = jax.random.split(jax.random.key(seed), 14)
    tokens = gaussian(key_of[0], (TOKENS, D), 1.0, 6.0, ((0, 32),))
    first_values = gaussian(key_of[1], (TOKENS, D), 1.0, 6.0, ((0, 32),))
    doc_lengths = jax.vmap(lambda own: ragged_sizes(own, NDOC, ROW, ROW // 2, 2))(jax.random.split(key_of[2], ROWS)).reshape((ROWS, NDOC)).astype(jnp.int32)
    cotangent = gaussian(key_of[3], (TOKENS, D), 1.0, 6.0, ((0, 32),))
    attn_gain = jnp.clip(1.0 + 0.15 * jax.random.normal(key_of[4], (D,), jnp.float32), 0.25, 1.75).astype(jnp.bfloat16)
    w_query = gaussian(key_of[5], (D, D), D ** -0.5, 0.1875, ((0, 32),))
    w_key = gaussian(key_of[6], (D, D), D ** -0.5, 0.1875, ((0, 32),))
    w_value = gaussian(key_of[7], (D, D), D ** -0.5, 0.1875, ((0, 32),))
    w_out = gaussian(key_of[8], (D, D), (D // 32) ** -0.5, 1.0, ((0, 32),))
    mlp_gain = jnp.clip(1.0 + 0.15 * jax.random.normal(key_of[9], (D,), jnp.float32), 0.25, 1.75).astype(jnp.bfloat16)
    w_gate = gaussian(key_of[10], (D, FF), D ** -0.5, 0.1875, ((1, 8),))
    w_up = gaussian(key_of[11], (D, FF), D ** -0.5, 0.1875, ((1, 8),))
    w_down = gaussian(key_of[12], (FF, D), FF ** -0.5, 0.109375, ((0, 8),))
    return dict(tokens=tokens, first_values=first_values, doc_lengths=doc_lengths, cotangent=cotangent, attn_gain=attn_gain, w_query=w_query, w_key=w_key, w_value=w_value, w_out=w_out, mlp_gain=mlp_gain, w_gate=w_gate, w_up=w_up, w_down=w_down)


epsilon = 1e-06
highest = lax.Precision.HIGHEST

@jax.custom_vjp
def low(v):
    return lax.optimization_barrier(v.astype(jnp.bfloat16)).astype(jnp.float32)

@jax.custom_vjp
def low_back(v):
    return v

def low_keep(v):
    return (low(v), None)

def low_pass(kept, grad):
    return (grad,)

def back_keep(v):
    return (v, None)

def back_low(kept, grad):
    return (low(grad),)
low.defvjp(low_keep, low_pass)
low_back.defvjp(back_keep, back_low)

def matmul_high(left_mat, right_mat):
    return jnp.dot(left_mat, right_mat, precision=highest)

def rms_scale(values, gain_vec):
    return values * lax.rsqrt(lax.optimization_barrier(jnp.mean(values * values, axis=-1, keepdims=True)) + epsilon) * gain_vec

def rope_tables(length, head_dim):
    half_dim = head_dim // 2
    places = jnp.arange(length).astype(jnp.float32)
    frequency = 10000.0 ** (-2.0 * jnp.arange(half_dim).astype(jnp.float32) / head_dim)
    angles = places[:, None] * frequency[None, :]
    return (jnp.cos(angles), jnp.sin(angles))

def rotate(values, cosine, sine_part):
    half_dim = values.shape[-1] // 2
    first_half = values[..., :half_dim]
    second_half = values[..., half_dim:]
    return jnp.concatenate([first_half * cosine - second_half * sine_part, second_half * cosine + first_half * sine_part], axis=-1)

def segment_ids(row_lengths, length):
    doc_ends = jnp.cumsum(row_lengths)
    places = jnp.arange(length).astype(jnp.int32)
    return lax.optimization_barrier(jnp.sum((places[:, None] >= doc_ends[None, :]).astype(jnp.int32), axis=-1)).astype(jnp.int32)

def layer_row(params, row_tokens, row_values, row_segments):
    attn_gain, w_query, w_key, w_value, w_out, mlp_gain, w_gate, w_up, w_down = params
    length = row_tokens.shape[0]
    normed = low(rms_scale(row_tokens, attn_gain))
    query_proj = low_back(matmul_high(normed, w_query))
    key_proj = low_back(matmul_high(normed, w_key))
    value_proj = low_back(matmul_high(normed, w_value))
    cosine, sine_part = rope_tables(length, HD)
    cosine = cosine[:, None, :]
    sine_part = sine_part[:, None, :]
    query_rot = low(rotate(query_proj.reshape(length, HEADS, HD), cosine, sine_part))
    key_rot = low(rotate(key_proj.reshape(length, HEADS, HD), cosine, sine_part))
    mixed_values = low(0.5 * value_proj + 0.5 * row_values).reshape(length, HEADS, HD)
    scores = low_back(jnp.einsum('qhd,khd->hqk', query_rot, key_rot, precision=highest) * HD ** (-0.5))
    places = jnp.arange(length)
    allowed = (row_segments[:, None] == row_segments[None, :]) & (places[:, None] >= places[None, :])
    scores = jnp.where(allowed[None], scores, -1e+30)
    row_max = lax.optimization_barrier(jnp.max(scores, axis=-1, keepdims=True))
    weights_exp = jnp.exp(scores - row_max)
    weights_soft = weights_exp / lax.optimization_barrier(jnp.sum(weights_exp, axis=-1, keepdims=True))
    attended = jnp.einsum('hqk,khd->qhd', low(weights_soft), mixed_values, precision=highest).reshape(length, HEADS * HD)
    attended = low_back(low(attended))
    branch = low_back(matmul_high(attended, w_out))
    middle = row_tokens + branch
    normed_two = low(rms_scale(middle, mlp_gain))
    gate_proj = low_back(matmul_high(normed_two, w_gate))
    up_proj = low_back(matmul_high(normed_two, w_up))
    hidden = low(jax.nn.silu(gate_proj) * up_proj)
    return middle + matmul_high(hidden, w_down)

def reference(tokens, first_values, doc_lengths, cotangent, attn_gain, w_query, w_key, w_value, w_out, mlp_gain, w_gate, w_up, w_down):
    segments = jax.vmap(lambda row_lengths: segment_ids(row_lengths, ROW))(doc_lengths)
    params = tuple((array_in.astype(jnp.float32) for array_in in (attn_gain, w_query, w_key, w_value, w_out, mlp_gain, w_gate, w_up, w_down)))

    def forward(param_set, tok_all, val_all):

        def one_row(row_items):
            return jax.checkpoint(layer_row)(param_set, row_items[0], row_items[1], row_items[2])
        outputs = lax.map(one_row, (tok_all.reshape(ROWS, ROW, D), val_all.reshape(ROWS, ROW, D), segments))
        return outputs.reshape(TOKENS, D)
    result, pullback = jax.vjp(forward, params, tokens.astype(jnp.float32), first_values.astype(jnp.float32))
    param_grads, token_grad, value_grad = pullback(cotangent.astype(jnp.float32))
    gain_one_grad, query_grad, key_grad, value_w_grad, out_grad, gain_two_grad, gate_grad, up_grad, down_grad = param_grads
    return (result.astype(jnp.bfloat16), token_grad.astype(jnp.bfloat16), value_grad.astype(jnp.bfloat16), query_grad, key_grad, value_w_grad, out_grad, gain_one_grad, gain_two_grad, gate_grad, up_grad, down_grad)
```

```python
import functools

import jax
import jax.numpy as jnp
from jax import lax
from jax.experimental import pallas as pl
from jax.experimental.pallas import tpu as pltpu
from jax.sharding import PartitionSpec as P


BF = jnp.bfloat16
F32 = jnp.float32
HD = 64
QB = 128
LONGEST = 512
NMAX = LONGEST // QB + 1
EPS = 1e-06
TB = 256
VMEM_ALL = 64 * 2**20 - 65536
AXES = ("dp", "hid", "dm")


def nt(a, b):
    return lax.dot_general(a, b, (((1,), (1,)), ((), ())), preferred_element_type=F32)


def nn(a, b):
    return lax.dot_general(a, b, (((1,), (0,)), ((), ())), preferred_element_type=F32)


def tn(a, b):
    return lax.dot_general(a, b, (((0,), (0,)), ((), ())), preferred_element_type=F32)


def swap(x, axis, mask):
    size = lax.axis_size(axis)
    return lax.ppermute(x, axis, [(i, i ^ mask) for i in range(size)])


class Plan:
    def __init__(self):
        self.ndp, self.nhid, self.ndm = (lax.axis_size(a) for a in AXES)
        hid = [("hid", 1 << b) for b in range(self.nhid.bit_length() - 1)]
        rest = [("dm", 1 << b) for b in range(self.ndm.bit_length() - 2, 0, -1)]
        self.core = ("dm", 1)
        self.order_a = hid + rest + [self.core]
        self.order_b = rest + hid + [self.core]

    def masks(self, order):
        out = [(0, 0)]
        for axis, mask in order:
            out += [(h ^ mask, d) if axis == "hid" else (h, d ^ mask) for h, d in out]
        return out

    def slab_order(self, order):
        return [(z, h, d) for h, d in self.masks(order) for z in range(self.ndp)]

    def device(self, z, h, d):
        me = [lax.axis_index(a) for a in AXES]
        return ((me[0] ^ z) * self.nhid + (me[1] ^ h)) * self.ndm + (me[2] ^ d)


def spread(piece, order):
    pieces = [piece]
    for axis, mask in order:
        pieces = pieces + [swap(p, axis, mask) for p in pieces]
    return pieces


def spread_dp(piece, ndp):
    return jnp.stack([piece] + [swap(piece, "dp", z) for z in range(1, ndp)])


def everywhere_sum(x):
    for axis in AXES:
        mask = 1
        while mask < lax.axis_size(axis):
            x = x + swap(x, axis, mask)
            mask *= 2
    return x


def bf_add(*terms):
    total = terms[0].astype(F32)
    for t in terms[1:]:
        total = total + t.astype(F32)
    return total


def first_head():
    return lax.broadcasted_iota(jnp.int32, (1, 128), 1) < HD


def split_pair(x, first):
    z = jnp.zeros_like(x)
    return jnp.concatenate([jnp.where(first, x, z), jnp.where(first, z, x)], axis=0)


def join_pair(x, first):
    h = x.shape[0] // 2
    return jnp.where(first, x[:h], x[h:])


def attn_fwd_kernel(low_ref, start_ref, q_ref, k_ref, v_ref, o_ref):
    row = pl.program_id(0)
    first = first_head()

    def step(i, _):
        rows = pl.ds(pl.multiple_of(i * QB, QB), QB)
        count = i - low_ref[row, i] + 1
        for n in range(1, NMAX + 1):

            @pl.when(count == n)
            def _():
                base = pl.multiple_of((i - (n - 1)) * QB, QB)
                keys = pl.ds(base, n * QB)
                q = split_pair(q_ref[rows, :] * jnp.asarray(HD**-0.5, BF), first)
                s = nt(q, k_ref[keys, :])
                st = start_ref[rows, :1] - base
                st = jnp.concatenate([st, st], axis=0)
                col = lax.broadcasted_iota(jnp.int32, s.shape, 1)
                me = lax.broadcasted_iota(jnp.int32, (2 * QB, 1), 0)
                me = jnp.where(me >= QB, me - QB, me) + (n - 1) * QB
                s = jnp.where((col >= st) & (col <= me), s, -1e30)
                p = jnp.exp(s - jnp.max(s, axis=1, keepdims=True))
                total = jnp.sum(p, axis=1, keepdims=True)
                p = (p * (1.0 / total)).astype(BF)
                o_ref[rows, :] = join_pair(nn(p, v_ref[keys, :]), first).astype(BF)

        return 0

    lax.fori_loop(0, q_ref.shape[0] // QB, step, 0)


def attn_fwd(low, start, q, k, v, rows):
    length = q.shape[0] // rows
    width = q.shape[1]
    spec = pl.BlockSpec((length, 128), lambda r, h, *_: (r, h))
    return pl.pallas_call(
        attn_fwd_kernel,
        out_shape=jax.ShapeDtypeStruct(q.shape, BF),
        grid_spec=pltpu.PrefetchScalarGridSpec(
            num_scalar_prefetch=1,
            grid=(rows, width // 128),
            in_specs=[pl.BlockSpec((length, 128), lambda r, h, *_: (r, 0)), spec, spec, spec],
            out_specs=spec,
        ),
        name="attn_fwd",
        cost_estimate=pl.CostEstimate(
            flops=30_000_000_000, bytes_accessed=8 * q.size, transcendentals=0
        ),
    )(low, start, q, k, v)


def attn_bwd_kernel(
    low_ref, start_ref, cos_ref, sin_ref, q_ref, k_ref, v_ref, g_ref,
    dq_ref, dk_ref, dv_ref, qa, ka, va,
):
    row = pl.program_id(0)
    first = first_head()
    ka[...] = jnp.zeros_like(ka)
    va[...] = jnp.zeros_like(va)

    def step(i, _):
        rows = pl.ds(pl.multiple_of(i * QB, QB), QB)
        count = i - low_ref[row, i] + 1
        for n in range(1, NMAX + 1):

            @pl.when(count == n)
            def _():
                base = pl.multiple_of((i - (n - 1)) * QB, QB)
                keys = pl.ds(base, n * QB)
                q = split_pair(q_ref[rows, :] * jnp.asarray(HD**-0.5, BF), first)
                g = split_pair(g_ref[rows, :], first)
                kb = k_ref[keys, :]
                s = nt(kb, q)
                st = start_ref[row, pl.ds(i, 1), :] - base
                st = jnp.concatenate([st, st], axis=1)
                me = lax.broadcasted_iota(jnp.int32, (1, 2 * QB), 1)
                me = jnp.where(me >= QB, me - QB, me) + (n - 1) * QB
                col = lax.broadcasted_iota(jnp.int32, s.shape, 0)
                s = jnp.where((col >= st) & (col <= me), s, -1e30)
                p = jnp.exp(s - jnp.max(s, axis=0, keepdims=True))
                p = p * (1.0 / jnp.sum(p, axis=0, keepdims=True))
                pd = p * nt(v_ref[keys, :], g)
                ds = (pd - p * jnp.sum(pd, axis=0, keepdims=True)).astype(BF)
                va[keys, :] += nn(p.astype(BF), g)
                ka[keys, :] += nn(ds, q)
                qa[rows, :] = join_pair(tn(ds, kb), first) * (HD**-0.5)

        return 0

    lax.fori_loop(0, q_ref.shape[0] // QB, step, 0)
    lower = (lax.broadcasted_iota(jnp.int32, (1, 128), 1) % HD) < HD // 2

    def back(x):
        other = jnp.where(lower, pltpu.roll(x, 128 - HD // 2, 1), pltpu.roll(x, HD // 2, 1))
        return (x * cos_ref[...] - other * sin_ref[...]).astype(BF)

    dq_ref[...] = back(qa[...])
    dk_ref[...] = back(ka[...])
    dv_ref[...] = (va[...] * 0.5).astype(BF)


def attn_bwd(low, start, cos, sin, q, k, v, g, rows):
    length = q.shape[0] // rows
    width = q.shape[1]
    spec = pl.BlockSpec((length, 128), lambda r, h, *_: (r, h))
    tab = pl.BlockSpec((length, 128), lambda r, h, *_: (0, 0))
    return pl.pallas_call(
        attn_bwd_kernel,
        out_shape=[jax.ShapeDtypeStruct(q.shape, BF)] * 3,
        grid_spec=pltpu.PrefetchScalarGridSpec(
            num_scalar_prefetch=1,
            grid=(rows, width // 128),
            in_specs=[pl.BlockSpec(start.shape, lambda r, h, *_: (0, 0, 0)), tab, tab]
            + [spec] * 4,
            out_specs=[spec] * 3,
            scratch_shapes=[pltpu.VMEM((length, 128), F32)] * 3,
        ),
        name="attn_bwd",
        cost_estimate=pl.CostEstimate(
            flops=40_000_000_000, bytes_accessed=14 * q.size, transcendentals=0
        ),
    )(low, start, cos, sin, q, k, v, g)


def doc_starts(doc_lengths, length):
    begins = jnp.cumsum(doc_lengths, axis=1) - doc_lengths
    place = jnp.arange(length, dtype=jnp.int32)
    inside = place[None, :, None] >= begins[:, None, :]
    return jnp.max(jnp.where(inside, begins[:, None, :], 0), axis=2)


def rope_tables(length):
    half = HD // 2
    places = jnp.arange(length).astype(F32)
    frequency = 10000.0 ** (-2.0 * jnp.arange(half).astype(F32) / HD)
    angles = places[:, None] * frequency[None, :]
    cos, sin = jnp.cos(angles), jnp.sin(angles)
    return jnp.tile(cos, (1, 128 // half)), jnp.tile(
        jnp.concatenate([-sin, sin], axis=1), (1, 128 // HD)
    )


def ffn_kernel(n_pieces, rows_each, tile, carry, *refs):
    refs = list(refs)
    n2, cot = refs.pop(0), refs.pop(0)
    if carry:
        oin, nin = refs.pop(0), refs.pop(0)
    pieces = [refs.pop(0) for _ in range(n_pieces)]
    n_tiles = n_pieces * rows_each // tile
    grads = [refs.pop(0) for _ in range(n_tiles)]
    oacc, nacc, w, ht, gt, ut, sems = refs
    t = pl.program_id(0)

    def copy(j):
        return pltpu.make_async_copy(
            pieces[j], w.at[:, pl.ds(j * rows_each, rows_each), :], sems.at[j]
        )

    @pl.when(t == 0)
    def _():
        for j in range(n_pieces):
            copy(j).start()
        if carry:
            oacc[...] = oin[...]
            nacc[...] = nin[...]
        else:
            oacc[...] = jnp.zeros_like(oacc)
            nacc[...] = jnp.zeros_like(nacc)

    done = 0
    for tt in range(n_tiles):
        need = -(-(tt + 1) * tile // rows_each)

        @pl.when(t == tt)
        def _(done=done, need=need):
            for j in range(done, need):
                copy(j).wait()

        done = need
    wrows = pl.ds(pl.multiple_of(t * tile, 16), tile)

    def block(b, _):
        rows = pl.ds(pl.multiple_of(b * TB, TB), TB)
        x = n2[rows, :]
        gate, up = nt(x, w[0, wrows, :]), nt(x, w[1, wrows, :])
        g = nt(cot[rows, :], w[2, wrows, :])
        sig = 1.0 / (1.0 + jnp.exp(-gate))
        silu = gate * sig
        hidden = (silu * up).astype(BF)
        dgate = (g * up * (sig + silu * (1.0 - sig))).astype(BF)
        dup = (g * silu).astype(BF)
        ht[:, rows] = hidden.T
        gt[:, rows] = dgate.T
        ut[:, rows] = dup.T
        oacc[rows, :] += nn(hidden, w[2, wrows, :])
        nacc[rows, :] += nn(dgate, w[0, wrows, :]) + nn(dup, w[1, wrows, :])
        return 0

    lax.fori_loop(0, n2.shape[0] // TB, block, 0)
    part = tile // 4
    for tt in range(n_tiles):

        @pl.when(t == tt)
        def _(tt=tt):
            def wblock(b, _):
                rows = pl.ds(pl.multiple_of(b * part, 16), part)
                grads[tt][0, rows, :] = nn(gt[rows, :], n2[...]).astype(BF)
                grads[tt][1, rows, :] = nn(ut[rows, :], n2[...]).astype(BF)
                grads[tt][2, rows, :] = nn(ht[rows, :], cot[...]).astype(BF)
                return 0

            lax.fori_loop(0, 4, wblock, 0)


def ffn(n2, cot, pieces, carry=None):
    tokens, width = n2.shape
    n, each = len(pieces), pieces[0].shape[1]
    total = n * each
    n_tiles = 2
    tile = total // n_tiles
    full = pl.BlockSpec((tokens, width), lambda t: (0, 0), pipeline_mode=pl.Buffered(1))
    out = pl.BlockSpec((3, tile, width), lambda t: (0, 0, 0), pipeline_mode=pl.Buffered(1))
    hbm = pl.BlockSpec(memory_space=pl.ANY)
    carried = [] if carry is None else list(carry)
    return pl.pallas_call(
        functools.partial(ffn_kernel, n, each, tile, carry is not None),
        out_shape=[jax.ShapeDtypeStruct((3, tile, width), BF)] * n_tiles
        + [jax.ShapeDtypeStruct((tokens, width), F32)] * 2,
        grid=(n_tiles,),
        in_specs=[full] * (2 + len(carried)) + [hbm] * n,
        out_specs=[out] * n_tiles + [full] * 2,
        scratch_shapes=[pltpu.VMEM((3, total, width), BF)]
        + [pltpu.VMEM((tile, tokens), BF)] * 3
        + [pltpu.SemaphoreType.DMA((n,))],
        input_output_aliases={2: n_tiles, 3: n_tiles + 1} if carried else {},
        compiler_params=pltpu.CompilerParams(vmem_limit_bytes=VMEM_ALL),
        name="ffn",
        cost_estimate=pl.CostEstimate(
            flops=18 * tokens * width * total,
            bytes_accessed=4 * (3 * total * width + 4 * tokens * width),
            transcendentals=0,
        ),
    )(n2, cot, *carried, *pieces)


class Slabs:
    def __init__(self, plan, masks, ndp, rows):
        self.plan, self.masks, self.ndp, self.rows = plan, masks, ndp, rows

    def copies(self, pieces, offset, count, dst, sem):
        out = []
        for piece, (h, d) in zip(pieces, self.masks):
            for z in range(self.ndp):
                if self.plan is None:
                    place = 0
                else:
                    place = pl.multiple_of(self.plan.device(z, h, d) * count, 16)
                out.append(
                    pltpu.make_async_copy(
                        piece.at[z, pl.ds(offset, count), :], dst.at[pl.ds(place, count), :], sem
                    )
                )
        return out


def start_all(copies):
    for c in copies:
        c.start()


def wait_whole(dst, sem):
    pltpu.make_async_copy(dst, dst, sem).wait()


def read_gains(n, ndp, rows, pieces, buf, sem, start):
    for i, piece in enumerate(pieces):
        c = pltpu.make_async_copy(piece.at[:, pl.ds(rows, 16), :], buf.at[i], sem.at[i])
        if start:
            c.start()
        else:
            c.wait()


def qkv_kernel(
    plan, masks_a, masks_b, ndp, count, n, tokens, first_values, cos_ref, sin_ref, *refs
):
    refs = list(refs)
    pa = [refs.pop(0) for _ in range(n)]
    pb = [refs.pop(0) for _ in range(n)]
    q_ref, k_ref, v_ref, nt_ref, wq, wk, wv, gains, buf, sems, gsems = refs
    a = Slabs(plan, masks_a, ndp, 2 * count)
    b = Slabs(plan, masks_b, ndp, 2 * count)
    start_all(a.copies(pa, 0, count, wq, sems.at[0]))
    start_all(a.copies(pa, count, count, wk, sems.at[1]))
    start_all(b.copies(pb, 0, count, wv, sems.at[2]))
    read_gains(n, ndp, 2 * count, pb, buf, gsems, True)
    read_gains(n, ndp, 2 * count, pb, buf, gsems, False)
    total = jnp.zeros(buf.shape[2:], F32)
    for i in range(n):
        for z in range(ndp):
            total = total + buf[i, z].astype(F32)
    gains[...] = total
    for i, w in enumerate((wq, wk, wv)):
        wait_whole(w, sems.at[i])
    lower = (lax.broadcasted_iota(jnp.int32, (1, 128), 1) % HD) < HD // 2
    width = tokens.shape[1]

    def block(i, _):
        rows = pl.ds(pl.multiple_of(i * TB, TB), TB)
        x = tokens[rows, :].astype(F32)
        r = lax.rsqrt(jnp.mean(x * x, axis=1, keepdims=True) + EPS)
        normed = (x * r * gains[0:1, :]).astype(BF)
        nt_ref[:, rows] = normed.T
        cos, sin = cos_ref[rows, :], sin_ref[rows, :]
        for w, out in ((wq, q_ref), (wk, k_ref)):
            y = nn(normed, w[...])
            for c in range(width // 128):
                part = y[:, c * 128 : (c + 1) * 128]
                other = jnp.where(
                    lower, pltpu.roll(part, 128 - HD // 2, 1), pltpu.roll(part, HD // 2, 1)
                )
                out[rows, c * 128 : (c + 1) * 128] = (part * cos + other * sin).astype(BF)
        v = nn(normed, wv[...])
        v_ref[rows, :] = (0.5 * v + 0.5 * first_values[rows, :].astype(F32)).astype(BF)
        return 0

    lax.fori_loop(0, tokens.shape[0] // TB, block, 0)


def whole(shape):
    zeros = (0,) * len(shape)
    return pl.BlockSpec(shape, lambda *_: zeros)


HBM = pl.BlockSpec(memory_space=pl.ANY)


def call(kernel, name, ins, outs, scratch, flops, spaces=None):
    spaces = spaces or [None] * len(ins)
    return pl.pallas_call(
        kernel,
        out_shape=[jax.ShapeDtypeStruct(s, t) for s, t in outs],
        in_specs=[HBM if s == "hbm" else pl.BlockSpec(memory_space=pltpu.VMEM) for s in spaces],
        out_specs=[pl.BlockSpec(memory_space=pltpu.VMEM) for _ in outs],
        scratch_shapes=scratch,
        compiler_params=pltpu.CompilerParams(vmem_limit_bytes=VMEM_ALL),
        name=name,
        cost_estimate=pl.CostEstimate(
            flops=flops, bytes_accessed=sum(2 * x.size for x in ins), transcendentals=0
        ),
    )(*ins)


def qkv(plan, masks_a, masks_b, ndp, count, tokens, first_values, cos, sin, pa, pb):
    n = len(pa)
    t, w = tokens.shape
    return call(
        functools.partial(qkv_kernel, plan, masks_a, masks_b, ndp, count, n),
        "qkv",
        [tokens, first_values, cos, sin, *pa, *pb],
        [((t, w), BF)] * 3 + [((w, t), BF)] + [((w, w), BF)] * 3 + [((16, w), F32)],
        [
            pltpu.VMEM((n, ndp, 16, w), BF),
            pltpu.SemaphoreType.DMA((3,)),
            pltpu.SemaphoreType.DMA((n,)),
        ],
        6 * t * w * w,
        [None] * 4 + ["hbm"] * (2 * n),
    )


def out_kernel(plan, masks, ndp, count, n, att, tokens, gains, *refs):
    refs = list(refs)
    pb = [refs.pop(0) for _ in range(n)]
    mid_ref, n2_ref, wo, sem = refs
    start_all(Slabs(plan, masks, ndp, 2 * count).copies(pb, count, count, wo, sem))
    wait_whole(wo, sem)

    def block(i, _):
        rows = pl.ds(pl.multiple_of(i * TB, TB), TB)
        mid = tokens[rows, :].astype(F32) + nn(att[rows, :], wo[...])
        mid_ref[rows, :] = mid
        r = lax.rsqrt(jnp.mean(mid * mid, axis=1, keepdims=True) + EPS)
        n2_ref[rows, :] = (mid * r * gains[1:2, :]).astype(BF)
        return 0

    lax.fori_loop(0, att.shape[0] // TB, block, 0)


def out_proj(plan, masks, ndp, count, att, tokens, gains, pb):
    n = len(pb)
    t, w = tokens.shape
    return call(
        functools.partial(out_kernel, plan, masks, ndp, count, n),
        "out_proj",
        [att, tokens, gains, *pb],
        [((t, w), F32), ((t, w), BF), ((w, w), BF)],
        [pltpu.SemaphoreType.DMA],
        2 * t * w * w,
        [None] * 3 + ["hbm"] * n,
    )


def norm_back(x, gain, e):
    r = lax.rsqrt(jnp.mean(x * x, axis=1, keepdims=True) + EPS)
    ge = gain * e
    coef = jnp.mean(x * ge, axis=1, keepdims=True) * (r * r * r)
    return r * ge - x * coef, e * (x * r)


def mid_kernel(mid, nacc, oacc, cot, gains, wo, out_ref, gm_ref, gb_ref, ga_ref, gg_ref):
    gg_ref[...] = jnp.zeros_like(gg_ref)

    def block(i, _):
        rows = pl.ds(pl.multiple_of(i * TB, TB), TB)
        m = mid[rows, :]
        out_ref[rows, :] = (m + oacc[rows, :]).astype(BF)
        gin, gterm = norm_back(m, gains[1:2, :], nacc[rows, :])
        gg_ref[...] += jnp.sum(gterm.reshape(TB // 8, 8, -1), axis=0)
        gm = cot[rows, :].astype(F32) + gin
        gm_ref[rows, :] = gm
        gb = gm.astype(BF)
        gb_ref[rows, :] = gb
        ga_ref[rows, :] = nt(gb, wo[...]).astype(BF)
        return 0

    lax.fori_loop(0, mid.shape[0] // TB, block, 0)


def mid_back(mid, nacc, oacc, cot, gains, wo):
    t, w = cot.shape
    return call(
        mid_kernel,
        "mid_back",
        [mid, nacc, oacc, cot, gains, wo],
        [((t, w), BF), ((t, w), F32), ((t, w), BF), ((t, w), BF), ((8, w), F32)],
        [],
        2 * t * w * w,
    )


def wgrad_kernel(plan, slabs, count, n, transposed, lhs, *refs):
    refs = list(refs)
    rhs = [refs.pop(0) for _ in range(n)]
    outs = [refs.pop(0) for _ in range(2 * n)]
    left = refs.pop(0)
    if not transposed:
        flat = refs.pop(0)
        t = lhs.shape[0]

        def turn(i, _):
            rows = pl.ds(pl.multiple_of(i * TB, TB), TB)
            flat[:, rows] = lhs[rows, :].T
            return 0

        lax.fori_loop(0, t // TB, turn, 0)
        source = flat
    else:
        source = lhs
    for i, (z, h, d) in enumerate(slabs):
        place = pl.multiple_of(plan.device(z, h, d) * count, 16)
        left[i * count : (i + 1) * count, :] = source[pl.ds(place, count), :]
    half = left.shape[0] // 2
    for side in (1, 0):

        def block(b, _):
            rows = pl.ds(pl.multiple_of(b * TB, TB), TB)
            x = left[pl.ds(pl.multiple_of(side * half + b * TB, TB), TB), :]
            for j in range(n):
                outs[2 * j + side][rows, :] = nn(x, rhs[j][...]).astype(BF)
            return 0

        lax.fori_loop(0, half // TB, block, 0)


def wgrad(plan, slabs, count, lhs, rhs, transposed):
    t, w = rhs[0].shape
    n = len(rhs)
    res = call(
        functools.partial(wgrad_kernel, plan, slabs, count, n, transposed),
        "wgrad",
        [lhs, *rhs],
        [((w // 2, w), BF)] * (2 * n),
        [pltpu.VMEM((w, t), BF)] + ([] if transposed else [pltpu.VMEM((w, t), BF)]),
        2 * n * t * w * w,
    )
    return [(res[2 * j], res[2 * j + 1]) for j in range(n)]


def in_kernel(tokens, gm, dq, dk, dv, wq, wk, wv, gains, tg_ref, gg_ref):
    gg_ref[...] = jnp.zeros_like(gg_ref)

    def block(i, _):
        rows = pl.ds(pl.multiple_of(i * TB, TB), TB)
        e = nt(dq[rows, :], wq[...]) + nt(dk[rows, :], wk[...]) + nt(dv[rows, :], wv[...])
        gin, gterm = norm_back(tokens[rows, :].astype(F32), gains[0:1, :], e)
        gg_ref[...] += jnp.sum(gterm.reshape(TB // 8, 8, -1), axis=0)
        tg_ref[rows, :] = (gm[rows, :] + gin).astype(BF)
        return 0

    lax.fori_loop(0, tokens.shape[0] // TB, block, 0)


def in_back(tokens, gm, dq, dk, dv, wq, wk, wv, gains):
    t, w = tokens.shape
    return call(
        in_kernel,
        "in_back",
        [tokens, gm, dq, dk, dv, wq, wk, wv, gains],
        [((t, w), BF), ((8, w), F32)],
        [],
        6 * t * w * w,
    )


def gather_attention(plan, fast, wq, wk, wv, wo, gain_one, gain_two):
    share = gain_one.shape[0]
    width = wq.shape[1]
    me = (lax.axis_index("dp") * plan.nhid + lax.axis_index("hid")) * plan.ndm + lax.axis_index(
        "dm"
    )
    own = jnp.zeros((16, width), BF)
    own = lax.dynamic_update_slice(
        own, jnp.stack([gain_one, gain_two]), (jnp.int32(0), me * share)
    )
    pack_a = jnp.concatenate([wq, wk])
    pack_b = jnp.concatenate([wv, wo, own])
    if fast:
        pa = spread(spread_dp(pack_a, plan.ndp), plan.order_a)
        pb = spread(spread_dp(pack_b, plan.ndp), plan.order_b)
        return pa, pb
    full = [lax.all_gather(w, AXES, axis=0, tiled=True) for w in (wq, wk, wv, wo)]
    own = everywhere_sum(own)
    pa = jnp.concatenate(full[:2])[None]
    pb = jnp.concatenate(full[2:] + [own])[None]
    return [pa], [pb]


def scatter_attention(plan, keep, send, order):
    got = swap(send, *plan.core)
    terms = [keep, got]
    axes = [s for s in plan.order_a if s != plan.core]
    steps = len(axes)
    shape = (2,) * steps + (plan.ndp, keep.shape[0] // (plan.ndp << steps), keep.shape[1])
    terms = [x.reshape(shape) for x in terms]
    left = list(range(steps - 1, -1, -1))
    for s in order:
        at = left.index(s)
        out = bf_add(*[lax.index_in_dim(x, 1, at, keepdims=False) for x in terms]).astype(BF)
        terms = [lax.index_in_dim(x, 0, at, keepdims=False) for x in terms]
        terms.append(swap(out, *axes[s]))
        left.pop(at)
    parts = [swap(bf_add(*[x[z] for x in terms]).astype(BF), "dp", z) for z in range(1, plan.ndp)]
    return bf_add(*[x[0] for x in terms], *parts)


def scatter_ffn(plan, keep, send, order):
    got = swap(send, *plan.core)
    terms = [keep, got]
    steps = [s for s in order if s != plan.core]
    for s in reversed(steps):
        half = terms[0].shape[1] // 2
        out = bf_add(*[x[:, half:] for x in terms]).astype(BF)
        terms = [x[:, :half] for x in terms]
        terms.append(swap(out, *s))
    total = bf_add(*terms)
    rows = total.shape[0] * total.shape[1]
    width = total.shape[2]
    each = -(-rows // (16 * plan.ndp)) * 16
    flat = total.reshape(rows, width)
    flat = jnp.pad(flat, ((0, each * plan.ndp - rows), (0, 0))).astype(BF)
    flat = flat.reshape(plan.ndp, each, width)
    me = lax.axis_index("dp")

    def part(z):
        return lax.dynamic_index_in_dim(flat, me ^ z, 0, keepdims=False)

    mine = bf_add(part(0), *[swap(part(z), "dp", z) for z in range(1, plan.ndp)]).astype(BF)
    others = [mine] + [swap(mine, "dp", z) for z in range(1, plan.ndp)]
    out = jnp.zeros((plan.ndp, each, width), BF)
    for z, x in enumerate(others):
        out = lax.dynamic_update_index_in_dim(out, x, me ^ z, 0)
    return out.reshape(plan.ndp * each, width)[:rows].reshape(total.shape)


def on_device(
    tokens, first_values, doc_lengths, cotangent, attn_gain, w_query, w_key, w_value, w_out,
    mlp_gain, w_gate, w_up, w_down,
):
    rows = doc_lengths.shape[0]
    tok_count, width = tokens.shape
    length = tok_count // rows
    plan = Plan()
    count = w_query.shape[0]
    units = w_down.shape[0]
    fast = count % 16 == 0 and units % 32 == 0

    pa, pb = gather_attention(
        plan, fast, w_query, w_key, w_value, w_out, attn_gain, mlp_gain
    )
    stack = jnp.stack([w_gate.T, w_up.T, w_down])
    if fast:
        half = units // 2
        ffn_a = spread(stack[:, :half], plan.order_a)
        ffn_b = spread(stack[:, half:], plan.order_b)
        masks_a, masks_b = plan.masks(plan.order_a), plan.masks(plan.order_b)
        where = (plan, masks_a, masks_b, plan.ndp, count)
        where_b = (plan, masks_b, plan.ndp, count)
    else:
        full = lax.all_gather(stack, ("hid", "dm"), axis=1, tiled=True)
        half = full.shape[1] // 2
        ffn_a, ffn_b = [full[:, :half]], [full[:, half:]]
        where = (None, [(0, 0)], [(0, 0)], 1, width)
        where_b = (None, [(0, 0)], 1, width)

    starts = doc_starts(doc_lengths, length)
    low = starts[:, ::QB] // QB
    start_col = jnp.broadcast_to(starts.reshape(-1, 1), (tok_count, 128))
    start_row = starts.reshape(rows, length // QB, QB)
    cos, sin = rope_tables(length)
    cos_all, sin_all = jnp.tile(cos, (rows, 1)), jnp.tile(sin, (rows, 1))

    q, k, v, normed_t, wq, wk, wv, gains = qkv(
        *where, tokens, first_values, cos_all, sin_all, pa, pb
    )
    att = attn_fwd(low, start_col, q, k, v, rows)
    middle, normed_two, wo = out_proj(*where_b, att, tokens, gains, pb)

    *grads_a, oacc, nacc = ffn(normed_two, cotangent, ffn_a)
    *grads_b, oacc, nacc = ffn(normed_two, cotangent, ffn_b, (oacc, nacc))
    output, grad_middle, grad_branch, grad_att, gain_two_part = mid_back(
        middle, nacc, oacc, cotangent, gains, wo
    )
    dq, dk, dv = attn_bwd(low, start_row, cos, sin, q, k, v, grad_att, rows)

    if fast:
        slabs = plan.slab_order(plan.order_a)
        o_pair = wgrad(plan, slabs, count, att, [grad_branch], False)[0]
        pairs = wgrad(plan, slabs, count, normed_t, [dq, dk, dv], True)
        forward, backward = list(range(len(plan.order_a) - 1)), None
        backward = forward[::-1]
        query_sum = scatter_attention(plan, *pairs[0], backward)
        key_sum = scatter_attention(plan, *pairs[1], forward)
        value_sum = scatter_attention(plan, *pairs[2], backward)
        out_sum = scatter_attention(plan, *o_pair, forward)
        sum_a = scatter_ffn(plan, *grads_a, plan.order_a)
        sum_b = scatter_ffn(plan, *grads_b, plan.order_b)
        sums = jnp.concatenate([sum_a, sum_b], axis=1).astype(F32)
    else:
        def summed(x):
            return lax.psum_scatter(x.astype(BF), AXES, scatter_dimension=0, tiled=True).astype(
                F32
            )

        query_sum, key_sum, value_sum = (summed(nn(normed_t, x)) for x in (dq, dk, dv))
        out_sum = summed(tn(att, grad_branch))
        grads = jnp.concatenate([*grads_a, *grads_b], axis=1)
        part = lax.psum_scatter(grads, ("hid", "dm"), scatter_dimension=1, tiled=True)
        sums = lax.psum(part, "dp").astype(F32)
    tokens_grad, gain_one_part = in_back(tokens, grad_middle, dq, dk, dv, wq, wk, wv, gains)

    share = attn_gain.shape[0]
    gain_parts = jnp.stack([jnp.sum(gain_one_part, axis=0), jnp.sum(gain_two_part, axis=0)])
    gain_sums = everywhere_sum(gain_parts)
    me = (lax.axis_index("dp") * plan.nhid + lax.axis_index("hid")) * plan.ndm + lax.axis_index(
        "dm"
    )
    gain_own = lax.dynamic_slice(gain_sums, (jnp.int32(0), me * share), (2, share))
    return (
        output,
        tokens_grad,
        dv,
        query_sum,
        key_sum,
        value_sum,
        out_sum,
        gain_own[0],
        gain_own[1],
        sums[0].T,
        sums[1].T,
        sums[2],
    )


def solution(mesh):
    rows, vec = P(AXES, None), P(AXES)
    cols, units = P(None, ("hid", "dm")), P(("hid", "dm"), None)
    return jax.shard_map(
        on_device,
        mesh=mesh,
        in_specs=(rows, rows, rows, rows, vec, rows, rows, rows, rows, vec, cols, cols, units),
        out_specs=(rows, rows, rows, rows, rows, rows, rows, vec, vec, cols, cols, units),
        check_vma=False,
    )
```
